8 devices in a mesh: dp: 1 (over z), tp: 8 (over x, y, core).
Axes of the slice: x: 2, y: 2, z: 1, core: 2. Of those that a mesh axis runs over, the one named last changes fastest.
Arguments:
- x: bfloat16 [4, 512, 12288], P('dp')
- gain_a: bfloat16 [12288], replicated
- wq: bfloat16 [12288, 12288], P(None, 'tp')
- wk: bfloat16 [12288, 1024], P(None, 'tp')
- wv: bfloat16 [12288, 1024], P(None, 'tp')
- wo: bfloat16 [12288, 12288], P('tp')
- gain_m: bfloat16 [12288], replicated
- w_gate: bfloat16 [12288, 33792], P(None, 'tp')
- w_up: bfloat16 [12288, 33792], P(None, 'tp')
- w_down: bfloat16 [33792, 12288], P('tp')
Outputs:
- output: bfloat16 [4, 512, 12288], P('dp')
All inputs are finite; a program needn't handle non-finite values.
Results may differ from the reference program's by a relative error of at most 0.017.
Values are sent between devices in bfloat16 or wider.
A program may use at most 2 GiB of HBM per device.

```python
import jax
import jax.numpy as jnp
from jax import lax

SEQUENCES = 4
TOKENS = 512
D = 12288
HEADS = 96
KV_HEADS = 8
HEAD = 128
FF = 33792
THETA = 10000


def setup_inputs(seed: int = 0, part: int = 0) -> dict:
    kx, ka, km, kq, kk, kv, ko, kg, ku, kd = jax.random.split(jax.random.key(seed), 10)

    def weights(key, rows, columns):
        return jax.random.normal(key, (rows, columns), jnp.float32) * rows**-0.5

    drawn = {
        "x": jax.random.normal(jax.random.fold_in(kx, part), (SEQUENCES, TOKENS, D), jnp.float32),
        "gain_a": 1 + 0.1 * jax.random.normal(ka, (D,), jnp.float32),
        "wq": 2 * weights(kq, D, HEADS * HEAD),
        "wk": 2 * weights(kk, D, KV_HEADS * HEAD),
        "wv": 4 * weights(kv, D, KV_HEADS * HEAD),
        "wo": weights(ko, HEADS * HEAD, D),
        "gain_m": 1 + 0.1 * jax.random.normal(km, (D,), jnp.float32),
        "w_gate": weights(kg, D, FF),
        "w_up": weights(ku, D, FF),
        "w_down": 3 * weights(kd, FF, D),
    }
    return {k: v.astype(jnp.bfloat16) for k, v in drawn.items()}


def normed(x, gain):
    wide = x.astype(jnp.float32)
    scale = lax.rsqrt(jnp.mean(wide * wide, -1, keepdims=True) + 1e-6)
    return (wide * scale * gain.astype(jnp.float32)).astype(jnp.bfloat16)


def turned(t, place, theta):
    half = t.shape[-1] // 2
    angle = place.astype(jnp.float32)[:, None] * theta ** (-jnp.arange(half, dtype=jnp.float32) / half)
    cos, sin = jnp.cos(angle)[:, None], jnp.sin(angle)[:, None]
    a, b = t[..., :half].astype(jnp.float32), t[..., half:].astype(jnp.float32)
    return jnp.concatenate([a * cos - b * sin, b * cos + a * sin], -1).astype(jnp.bfloat16)


def matmul(a, w):
    return jnp.dot(a, w, preferred_element_type=jnp.float32).astype(jnp.bfloat16)


def einsum(form, a, b):
    return jnp.einsum(form, a.astype(jnp.float32), b.astype(jnp.float32))


def attention(q, k, v):
    scores = einsum("tgsd,ugd->gstu", q, k) * q.shape[-1] ** -0.5
    token = jnp.arange(q.shape[0])
    scores = jnp.where(token[:, None] >= token, scores, -jnp.inf)
    weights = jax.nn.softmax(scores, -1).astype(jnp.bfloat16)
    return einsum("gstu,ugd->tgsd", weights, v).astype(jnp.bfloat16)


def one(x, gain_a, wq, wk, wv, wo, gain_m, w_gate, w_up, w_down):
    rows = x.shape[0]
    a, place = normed(x, gain_a), jnp.arange(rows)
    k = turned(matmul(a, wk).reshape(rows, -1, HEAD), place, THETA)
    q = turned(matmul(a, wq).reshape(rows, -1, HEAD), place, THETA).reshape(rows, k.shape[1], -1, HEAD)
    v = matmul(a, wv).reshape(rows, -1, HEAD)
    seen = attention(q, k, v).reshape(rows, -1)
    h = (x.astype(jnp.float32) + jnp.dot(seen, wo, preferred_element_type=jnp.float32)).astype(jnp.bfloat16)
    b = normed(h, gain_m)
    gate = jnp.dot(b, w_gate, preferred_element_type=jnp.float32)
    up = jnp.dot(b, w_up, preferred_element_type=jnp.float32)
    hidden = (jax.nn.silu(gate) * up).astype(jnp.bfloat16)
    return (h.astype(jnp.float32) + jnp.dot(hidden, w_down, preferred_element_type=jnp.float32)).astype(jnp.bfloat16)


def reference(x, gain_a, wq, wk, wv, wo, gain_m, w_gate, w_up, w_down):
    return lax.map(lambda sequence: one(sequence, gain_a, wq, wk, wv, wo, gain_m, w_gate, w_up, w_down), x)
```

```python
import functools

import jax
import jax.numpy as jnp
from jax import lax
from jax.experimental import pallas as pl
from jax.experimental.pallas import tpu as pltpu
from jax.sharding import PartitionSpec as P

HEAD = 128
THETA = 10000
QUERIES = 256


def normed(x, gain):
    wide = x.astype(jnp.float32)
    scale = lax.rsqrt(jnp.mean(wide * wide, -1, keepdims=True) + 1e-6)
    return (wide * scale * gain.astype(jnp.float32)).astype(jnp.bfloat16)


def tables(rows):
    half = HEAD // 2
    angle = jnp.arange(rows).astype(jnp.float32)[:, None] * THETA ** (-jnp.arange(half, dtype=jnp.float32) / half)
    cos, sin = jnp.cos(angle), jnp.sin(angle)
    return jnp.concatenate([cos, cos], -1), jnp.concatenate([-sin, sin], -1)


def attention_kernel(cos_ref, sin_ref, q_ref, kv_ref, o_ref, k_s):
    rows = q_ref.shape[0]

    def turned(t):
        wide = t.astype(jnp.float32)
        return (wide * cos_ref[...] + pltpu.roll(wide, HEAD // 2, 1) * sin_ref[...]).astype(jnp.bfloat16)

    @pl.when(pl.program_id(1) == 0)
    def _():
        k_s[...] = turned(kv_ref[:, :HEAD])

    for n in range(q_ref.shape[1] // HEAD):
        q = turned(q_ref[:, n * HEAD : (n + 1) * HEAD])
        for first in range(0, rows, QUERIES):
            keys = first + QUERIES
            s = lax.dot_general(q[first:keys], k_s[:keys], (((1,), (1,)), ((), ())), preferred_element_type=jnp.float32) * HEAD**-0.5
            seen = first + lax.broadcasted_iota(jnp.int32, s.shape, 0) >= lax.broadcasted_iota(jnp.int32, s.shape, 1)
            s = jnp.where(seen, s, -jnp.inf)
            p = jnp.exp(s - s.max(-1, keepdims=True))
            p = (p * (1 / p.sum(-1, keepdims=True))).astype(jnp.bfloat16)
            out = jnp.dot(p, kv_ref[:keys, HEAD:], preferred_element_type=jnp.float32)
            o_ref[first:keys, n * HEAD : (n + 1) * HEAD] = out.astype(jnp.bfloat16)


def attention(q, kv, rows, cos, sin, group=4):
    tokens, width = q.shape
    wide = group * HEAD
    table = pl.BlockSpec((rows, HEAD), lambda b, h: (0, 0))
    heads = pl.BlockSpec((rows, wide), lambda b, h: (b, h))
    return pl.pallas_call(
        attention_kernel,
        grid=(tokens // rows, width // wide),
        in_specs=[table, table, heads, pl.BlockSpec((rows, 2 * HEAD), lambda b, h: (b, 0))],
        out_specs=heads,
        out_shape=jax.ShapeDtypeStruct(q.shape, jnp.bfloat16),
        scratch_shapes=[pltpu.VMEM((rows, HEAD), jnp.bfloat16)],
        compiler_params=pltpu.CompilerParams(dimension_semantics=("parallel", "arbitrary"), vmem_limit_bytes=32 * 2**20),
        cost_estimate=pl.CostEstimate(flops=4 * tokens * rows * width, transcendentals=tokens * rows * width // HEAD, bytes_accessed=4 * tokens * width),
    )(cos, sin, q, kv)


def solution(mesh):
    n = mesh.shape["tp"]

    def dot(a, w):
        return jnp.dot(a, w, preferred_element_type=jnp.float32)

    def scattered(term):
        return lax.psum_scatter(term.astype(jnp.bfloat16), "tp", scatter_dimension=0, tiled=True)

    def gathered(own):
        return lax.all_gather(own, "tp", axis=0, tiled=True)

    def step(x, gain_a, wq, wk, wv, wo, gain_m, w_gate, w_up, w_down):
        batch, rows, d = x.shape
        flat = x.reshape(batch * rows, d)
        cos, sin = tables(rows)
        wkv = jnp.concatenate([wk, wv], 1)
        me = lax.axis_index("tp")

        count = rows
        own, total = count // n, batch * rows

        def tied(*values):
            return lax.optimization_barrier(values)

        def swapped(t, bit):
            return lax.ppermute(t, "tp", [(j, j ^ bit) for j in range(n)])

        def near(i):
            y = (h[i].astype(jnp.float32) + late[i].astype(jnp.float32)).astype(jnp.bfloat16)
            return y, swapped(y, 4), swapped(y, 2)

        def far(y, over_x, over_y):
            return y, over_x, over_y, swapped(over_y[: own // 2], 4), swapped(over_x[own // 2 :], 2)

        def placed(out, i, blocks):
            for block, bits, shift in zip(blocks, (0, 4, 2, 6, 6), (0, 0, 0, 0, own // 2)):
                for bit, piece in ((0, block), (1, swapped(block, 1))):
                    at = i * count + jnp.bitwise_xor(me, bits + bit) * own + shift
                    out = lax.dynamic_update_slice_in_dim(out, piece, at, axis=0)
            return out

        sums, h, b, late, blocks = ([None] * batch for _ in range(5))

        def joined(i, work):
            work, sums[i] = tied(work, sums[i])
            mine = lax.dynamic_slice_in_dim(flat, i * count + me * own, own, axis=0)
            h[i] = (mine.astype(jnp.float32) + sums[i].astype(jnp.float32)).astype(jnp.bfloat16)
            work, normal = tied(work, normed(h[i], gain_m))
            b[i] = gathered(normal)
            return work

        gain = gain_a
        for i in range(batch):
            a = normed(lax.slice_in_dim(flat, i * count, (i + 1) * count, axis=0), gain)
            q, kv = dot(a, wq).astype(jnp.bfloat16), dot(a, wkv).astype(jnp.bfloat16)
            if i >= 2:
                q = joined(i - 2, q)
            term = dot(attention(q, kv, rows, cos, sin), wo).astype(jnp.bfloat16)
            sums[i] = scattered(term)
            gain, _ = tied(gain_a, term)

        out = jnp.zeros_like(flat)
        for i in range(batch):
            b[i], _ = tied(b[i], term)
            gate = dot(b[i], w_gate)
            if i < 2:
                gate = joined(batch - 2 + i, gate)
            else:
                gate, late[i - 2] = tied(gate, late[i - 2])
                first = near(i - 2)
                gate, own_y = tied(gate, first[0])
                blocks[i - 2] = (own_y, *first[1:])
            hidden = (jax.nn.silu(gate) * dot(b[i], w_up)).astype(jnp.bfloat16)
            if i >= 2:
                hidden, *exchanged = tied(hidden, *blocks[i - 2])
                blocks[i - 2] = far(*exchanged)
            term = dot(hidden, w_down).astype(jnp.bfloat16)
            late[i] = scattered(term)
            if i >= 2:
                out = placed(out, i - 2, tied(term, *blocks[i - 2])[1:])
        for i in range(batch - 2, batch):
            out = placed(out, i, far(*near(i)))
        return out.reshape(x.shape)

    tokens, whole, columns, rows_of = P("dp", None, None), P(None), P(None, "tp"), P("tp", None)
    return jax.shard_map(
        step,
        mesh=mesh,
        in_specs=(tokens, whole, columns, columns, columns, rows_of, whole, columns, columns, rows_of),
        out_specs=tokens,
        check_vma=False,
    )
```
